32 devices in a mesh: band: 8 (over z, x), dir: 4 (over y, core).
Axes of the slice: x: 2, y: 2, z: 4, core: 2. Of those that a mesh axis runs over, the one named last changes fastest.
Arguments:
- visibilities: bfloat16 [16, 32, 2, 256, 256], P('band', 'dir'), as said below
- sky_model: bfloat16 [16, 32, 2, 256, 256], P('band', 'dir')
- rfi_flags: int32 [16, 8, 8], P('band'), may hold values from 0 to 1, as said below
- destination: int32 [16], P('band'), may hold values from 0 to 15, as said below
Outputs:
- delivered: float32 [16, 32, 2, 256], P('band', 'dir')
- coefficients: float32 [9, 32, 2, 256], P(None, 'dir')
- norm_values: float32 [2, 2], replicated
The draws below stay inside these ranges and needn't reach their ends.
Inputs may be any that keep to these rules, and one draw needn't show every extreme that they name: `rfi_flags`: 1 marks a flagged baseline block; the share of flagged blocks tends to fall with the subband index. destination holds every row of 0 to 15 once. With the rows split into 8 aligned blocks of 2 rows, one row of block i goes to a row of block i + 1 and the other to a row of block i + 4, modulo 16 // 2. `visibilities`: visibilities follow the model under unknown station gains, with noise.
All inputs are finite; a program needn't handle non-finite values.
Results may differ from the reference program's by a relative error of at most 0.0003.
Values sent between devices are 32-bit elements; how exact they have to be, the bound alone decides.
A program may use at most 128 MiB of HBM per device.

```python
import jax
import jax.numpy as jnp
from jax import lax

STATIONS = 256
DIRECTIONS = 32
BLOCK = 32
DEGREE = 8
SWEEPS = 4
ITERS = 2
SB_DEV = 2
SUBBANDS = 16


def band_pair(key, band_row):
    band_key = jax.random.fold_in(jax.random.fold_in(key, 11), band_row)
    model_key, noise_key, rough_key = jax.random.split(band_key, 3)
    shared = jax.random.normal(jax.random.fold_in(key, 23), (4, DIRECTIONS, STATIONS), jnp.float32)
    rough = jax.random.normal(rough_key, (2, DIRECTIONS, STATIONS), jnp.float32)
    abscissa = (2.0 * band_row.astype(jnp.float32) + 1.0) / SUBBANDS - 1.0
    sky_values = jax.random.normal(model_key, (DIRECTIONS, 2, STATIONS, STATIONS), jnp.float32)
    noise_level = 0.5
    amp_spread = 0.25
    amplitude = 1.0 + amp_spread * shared[0] + 0.15 * abscissa * shared[1] + 0.1 * rough[0]
    phase = 0.8 * shared[2] + 0.5 * abscissa * shared[3] + 0.2 * rough[1]
    gain_re = amplitude * jnp.cos(phase)
    gain_im = amplitude * jnp.sin(phase)
    model_re = sky_values[:, 0]
    model_im = sky_values[:, 1]
    twist_re = model_re * gain_re[:, None, :] + model_im * gain_im[:, None, :]
    twist_im = model_im * gain_re[:, None, :] - model_re * gain_im[:, None, :]
    noise = jax.random.normal(noise_key, (2, DIRECTIONS, STATIONS, STATIONS), jnp.float32)
    data_re = gain_re[:, :, None] * twist_re - gain_im[:, :, None] * twist_im + noise_level * noise[0]
    data_im = gain_re[:, :, None] * twist_im + gain_im[:, :, None] * twist_re + noise_level * noise[1]
    return (sky_values.astype(jnp.bfloat16), jnp.stack([data_re, data_im], axis=1).astype(jnp.bfloat16))


def draw_sky_model(key, part):

    def one_band(band_row):
        return band_pair(key, band_row)[0]
    return lax.map(one_band, jnp.arange(SUBBANDS))


def draw_visibilities(key, part):

    def one_band(band_row):
        return band_pair(key, band_row)[1]
    return lax.map(one_band, jnp.arange(SUBBANDS))


def draw_rfi_flags(key, part):
    band_rows = jnp.arange(SUBBANDS)
    threshold = 750 - 600 * band_rows // max(SUBBANDS - 1, 1)
    blocks = STATIONS // BLOCK
    random_ints = jax.random.randint(jax.random.fold_in(key, 5), (SUBBANDS, blocks, blocks), 0, 1000)
    return (random_ints < threshold[:, None, None]).astype(jnp.int32)


def draw_destination(key, part):
    block_count = SUBBANDS // SB_DEV
    half_count = block_count // 2
    base_key = jax.random.fold_in(key, 7)
    send_key, recv_key = jax.random.split(base_key)
    send_perm = jax.vmap(lambda one_key: jax.random.permutation(one_key, SB_DEV))(jax.random.split(send_key, block_count))
    recv_perm = jax.vmap(lambda one_key: jax.random.permutation(one_key, SB_DEV))(jax.random.split(recv_key, block_count))
    block_ids = jnp.arange(block_count)[:, None]
    slot_ids = jnp.arange(SB_DEV)[None, :]
    source_rows = block_ids * SB_DEV + send_perm
    target_block = jnp.where(slot_ids == 0, (block_ids + 1) % block_count, jnp.where(slot_ids == 1, (block_ids + half_count) % block_count, block_ids + 0 * slot_ids))
    target_slot = recv_perm[target_block, slot_ids + 0 * block_ids]
    target_rows = target_block * SB_DEV + target_slot
    result = jnp.zeros((SUBBANDS,), jnp.int32).at[source_rows.reshape(-1)].set(target_rows.reshape(-1).astype(jnp.int32))
    return result.astype(jnp.int32)


def setup_inputs(seed: int = 0) -> dict:
    streams_of = jax.random.split(jax.random.key(seed), 5)
    return {
        "visibilities": draw_visibilities(jax.random.fold_in(streams_of[4], 71), 0),
        "sky_model": draw_sky_model(jax.random.fold_in(streams_of[4], 71), 0),
        "rfi_flags": draw_rfi_flags(jax.random.fold_in(streams_of[4], 71), 0),
        "destination": draw_destination(jax.random.fold_in(streams_of[4], 71), 0),
    }


highest = lax.Precision.HIGHEST
penalty_share = 0.4

def block_weights(rfi_flags):
    blocks = rfi_flags.shape[-1]
    kept_blocks = (1 - rfi_flags).astype(jnp.float32)
    leading = kept_blocks.shape[:-2]
    spread = jnp.broadcast_to(kept_blocks[..., :, None, :, None], leading + (blocks, BLOCK, blocks, BLOCK))
    stations = blocks * BLOCK
    spread = spread.reshape(leading + (stations, stations))
    return spread * (1.0 - jnp.eye(stations, dtype=jnp.float32))

def operators(visibilities, sky_model, rfi_flags):
    baseline = block_weights(rfi_flags)[..., None, :, :]
    data_re = visibilities[..., 0, :, :].astype(jnp.float32)
    data_im = visibilities[..., 1, :, :].astype(jnp.float32)
    model_re = sky_model[..., 0, :, :].astype(jnp.float32)
    model_im = sky_model[..., 1, :, :].astype(jnp.float32)
    oper_re = baseline * (model_re * data_re + model_im * data_im)
    oper_im = baseline * (model_re * data_im - model_im * data_re)
    square = baseline * (model_re * model_re + model_im * model_im)
    return (jnp.stack([oper_re, oper_im], axis=-3), square)

def chebyshev(band_rows, band_total):
    abscissa = (2.0 * band_rows + 1.0) / band_total - 1.0
    cheb_terms = [jnp.ones_like(abscissa), abscissa]
    for degree in range(2, DEGREE + 1):
        cheb_terms.append(2.0 * abscissa * cheb_terms[-1] - cheb_terms[-2])
    return jnp.stack(cheb_terms[:DEGREE + 1], axis=0)

def stefcal(operator, square, gain_now, target, penalty):
    pen_term = penalty[..., None, None, None]
    for sweep_index in range(SWEEPS):
        products = jnp.einsum('...kapq,...kbq->...kabp', operator, gain_now, precision=highest)
        real_part = products[..., 0, 0, :] - products[..., 1, 1, :]
        imag_part = products[..., 0, 1, :] + products[..., 1, 0, :]
        numerator = jnp.stack([real_part, imag_part], axis=-2)
        magnitude = lax.optimization_barrier(jnp.sum(gain_now * gain_now, axis=-2))
        denominator = jnp.einsum('...kpq,...kq->...kp', square, magnitude, precision=highest)
        updated = (numerator + pen_term * target) / (denominator[..., None, :] + pen_term)
        gain_now = 0.5 * (updated + gain_now) if sweep_index % 2 == 1 else updated
    return gain_now

def per_band(band_items):
    vis_band, model_band, flag_band, gain_band, target_band, pen_band = band_items
    operator, square = operators(vis_band, model_band, flag_band)
    return stefcal(operator, square, gain_band, target_band, pen_band)

def reference(visibilities, sky_model, rfi_flags, destination):
    band_total = visibilities.shape[0]
    directions = visibilities.shape[1]
    stations = visibilities.shape[-1]
    blocks = rfi_flags.shape[-1]
    weights = (1.0 + lax.optimization_barrier(jnp.sum(1 - rfi_flags, axis=(1, 2))).astype(jnp.float32)) / (1.0 + blocks * blocks)
    penalty = penalty_share * stations * weights
    cheb_basis = chebyshev(jnp.arange(band_total).astype(jnp.float32), band_total)
    weighted = cheb_basis * weights[None, :]
    gram_matrix = jnp.dot(weighted, cheb_basis.T, precision=highest)
    factor = jnp.linalg.cholesky(gram_matrix)
    normalizer = directions * 2.0 * stations * gram_matrix[0, 0]
    ones_part = jnp.ones((band_total, directions, stations), jnp.float32)
    unit_gains = jnp.stack([ones_part, jnp.zeros_like(ones_part)], axis=2)
    gain_now = unit_gains
    consensus = unit_gains
    dual_var = jnp.zeros_like(unit_gains)
    row_weight = weights[:, None, None, None]
    norm_rows = []
    coefficients = None
    for iteration in range(ITERS):
        gain_now = lax.map(per_band, (visibilities, sky_model, rfi_flags, gain_now, consensus - dual_var, penalty))
        projection = jnp.einsum('cs,skap->ckap', weighted, gain_now + dual_var, precision=highest)
        flat_proj = projection.reshape(projection.shape[0], -1)
        coefficients = jax.scipy.linalg.cho_solve((factor, True), flat_proj).reshape(projection.shape)
        fresh_gains = jnp.einsum('cs,ckap->skap', cheb_basis, coefficients, precision=highest)
        dual_var = dual_var + gain_now - fresh_gains
        primal = jnp.sqrt(jnp.sum(row_weight * (gain_now - fresh_gains) ** 2) / normalizer)
        dual_norm = jnp.sqrt(jnp.sum(row_weight * (fresh_gains - consensus) ** 2) / normalizer)
        norm_rows.append(jnp.stack([primal, dual_norm]))
        consensus = fresh_gains
    delivered = jnp.zeros_like(gain_now).at[destination].set(gain_now)
    return (delivered, coefficients, jnp.stack(norm_rows))
```

```python
import functools

import jax
import jax.numpy as jnp
from jax import lax
from jax.experimental import pallas as pl
from jax.experimental.pallas import tpu as pltpu
from jax.sharding import PartitionSpec as P

BLOCK = 32
DEGREE = 8
SWEEPS = 4
ITERS = 2
TERMS = DEGREE + 1
ROWS = 16
LANES = 128

penalty_share = 0.4
f32 = jnp.float32
bf16 = jnp.bfloat16
MESH = pl.DeviceIdType.MESH


def row_of(shape, axis=0):
    return lax.broadcasted_iota(jnp.int32, shape, axis)


def spread(value, shape):
    return jnp.broadcast_to(value, shape)


def left_side(gain):
    row = row_of(gain.shape)
    part = lax.rem(row, 4)
    re = spread(gain[0:1], gain.shape)
    im = spread(gain[1:2], gain.shape)
    zero = jnp.zeros_like(gain)
    first = jnp.where(part == 0, re, jnp.where(part == 1, im, zero))
    second = jnp.where(part == 0, -im, jnp.where(part == 1, re, zero))
    third = jnp.where(part == 2, re * re + im * im, zero)
    sides = []
    for full in (first, second, third):
        lead = full.astype(bf16).astype(f32)
        sides.append(jnp.where(row < 4, lead, full - lead).astype(bf16))
    return jnp.concatenate(sides + sides, axis=1)


def kernel(
    bands,
    dirs,
    vis_hbm,
    sky_hbm,
    flags,
    dest,
    delivered,
    coef,
    norms,
    vis,
    sky,
    oper,
    turned,
    keep,
    wpen,
    meta,
    gains,
    zall,
    uall,
    gtile,
    ttile,
    solve_rows,
    cheb_rows,
    norm_all,
    vis_sem,
    sky_sem,
    meta_send,
    meta_recv,
    gain_send,
    gain_recv,
    norm_send,
    norm_recv,
):
    subs, count, _, stations, _ = vis_hbm.shape
    blocks = flags.shape[-1]
    total = bands * subs
    width = meta.shape[-1]
    me = lax.axis_index("band")
    my_dir = lax.axis_index("dir")
    tile = (8, stations)

    def ahead(distance):
        return lax.rem(me + distance, bands)

    def behind(distance):
        return lax.rem(me + bands - distance, bands)

    def load(pair):
        s, k = divmod(pair, count)
        return (
            pltpu.make_async_copy(vis_hbm.at[s, k], vis.at[pair], vis_sem.at[pair]),
            pltpu.make_async_copy(sky_hbm.at[s, k], sky.at[pair], sky_sem.at[pair]),
        )

    for pair in range(subs * count):
        for copy in load(pair):
            copy.start()

    barrier = pltpu.get_barrier_semaphore()
    for distance in range(1, bands):
        pl.semaphore_signal(
            barrier, inc=1, device_id={"band": ahead(distance)}, device_id_type=MESH
        )
    for distance in range(1, dirs):
        pl.semaphore_signal(
            barrier,
            inc=1,
            device_id={"dir": lax.rem(my_dir + distance, dirs)},
            device_id_type=MESH,
        )

    lane_w = row_of((1, width), 1)
    weight_row = jnp.zeros((1, width), f32)
    dest_rows = []
    for s in range(subs):
        kept = (1 - flags[s]).astype(f32)
        weight = (1.0 + jnp.sum(kept, axis=(0, 1), keepdims=True)) / (1.0 + blocks * blocks)
        wpen[s] = spread(penalty_share * stations * weight, tile)
        weight_row = jnp.where(lane_w == me * subs + s, weight, weight_row)
        dest_rows.append(jnp.full((1, width), dest[s], jnp.int32).astype(f32))
        lane = row_of((1, stations), 1) // BLOCK
        for i in range(blocks):
            shape = (BLOCK, stations)
            across = jnp.zeros((1, stations), f32)
            for j in range(blocks):
                across = jnp.where(lane == j, kept[j : j + 1, i : i + 1], across)
            apart = row_of(shape) + i * BLOCK != row_of(shape, 1)
            keep[s, i * BLOCK : (i + 1) * BLOCK, :] = jnp.where(
                apart, spread(across, shape), 0.0
            )
    meta[me] = jnp.zeros(meta.shape[1:], f32)
    for s in range(subs):
        meta[me, s : s + 1, :] = dest_rows[s]
    meta[me, subs : subs + 1, :] = weight_row

    row = row_of(tile)
    for pair in range(subs * count):
        unit = jnp.where(row == 0, 1.0, jnp.zeros(tile, f32))
        gtile[pair] = unit
        ttile[pair] = unit

    pl.semaphore_wait(barrier, bands - 1 + dirs - 1)

    def meta_copy(slot, distance):
        return pltpu.make_async_remote_copy(
            src_ref=meta.at[slot],
            dst_ref=meta.at[slot],
            send_sem=meta_send.at[distance],
            recv_sem=meta_recv.at[distance],
            device_id={"band": ahead(distance)},
            device_id_type=MESH,
        )

    def gain_copy(it, slot, s, distance):
        return pltpu.make_async_remote_copy(
            src_ref=gains.at[it, slot, s],
            dst_ref=gains.at[it, slot, s],
            send_sem=gain_send.at[it, s, distance],
            recv_sem=gain_recv.at[it, s, distance],
            device_id={"band": ahead(distance)},
            device_id_type=MESH,
        )

    def norm_copy(slot, distance):
        return pltpu.make_async_remote_copy(
            src_ref=norm_all.at[slot],
            dst_ref=norm_all.at[slot],
            send_sem=norm_send.at[distance],
            recv_sem=norm_recv.at[distance],
            device_id={"dir": lax.rem(my_dir + distance, dirs)},
            device_id_type=MESH,
        )

    for distance in range(1, bands):
        meta_copy(me, distance).start()

    square = (stations, stations)
    identity = (row_of(square) == row_of(square, 1)).astype(f32).astype(bf16)

    def build(s):
        def one(k, carry):
            pair = s * count + k
            pltpu.make_async_copy(vis_hbm.at[s, k], vis.at[pair], vis_sem.at[pair]).wait()
            pltpu.make_async_copy(sky_hbm.at[s, k], sky.at[pair], sky_sem.at[pair]).wait()
            slot = lax.rem(k, 2)
            for part, source in enumerate((vis, sky)):
                for j in range(2):
                    turned[slot, 2 * part + j] = lax.dot_general(
                        identity,
                        source[pair, j],
                        (((1,), (1,)), ((), ())),
                        preferred_element_type=f32,
                    )
            for i in range(stations // BLOCK):
                rows = slice(i * BLOCK, (i + 1) * BLOCK)
                baseline = keep[s, rows, :]
                data_re = turned[slot, 0, rows, :]
                data_im = turned[slot, 1, rows, :]
                model_re = turned[slot, 2, rows, :]
                model_im = turned[slot, 3, rows, :]
                parts = (
                    baseline * (model_re * data_re + model_im * data_im),
                    baseline * (model_re * data_im - model_im * data_re),
                    baseline * (model_re * model_re + model_im * model_im),
                )
                for j, full in enumerate(parts):
                    lead = full.astype(bf16)
                    base = j * stations + i * BLOCK
                    oper[pair, base : base + BLOCK, :] = lead
                    base = base + 3 * stations
                    oper[pair, base : base + BLOCK, :] = (full - lead.astype(f32)).astype(bf16)
            return carry

        lax.fori_loop(0, count, one, 0, unroll=2)

    def sweeps(it, s):
        penalty = wpen[s]

        def one(index, held):
            step = jnp.where(lax.rem(index, 2) == 1, 0.5, 1.0).astype(f32)
            fresh = []
            for k in range(count):
                pair = s * count + k
                gain = held[k]
                out = lax.dot_general(
                    left_side(gain),
                    oper[pair],
                    (((1,), (0,)), ((), ())),
                    preferred_element_type=f32,
                )
                out = out + pltpu.roll(out, 4, 0)
                updated = (out + penalty * ttile[pair]) / (spread(out[2:3], tile) + penalty)
                fresh.append(step * updated + (1.0 - step) * gain)
            return tuple(fresh)

        start = tuple(gtile[s * count + k] for k in range(count))
        final = lax.fori_loop(0, SWEEPS, one, start)
        for k in range(count):
            gtile[s * count + k] = final[k]
            gains[it, me, s, k : k + 1, 0:stations] = final[k][0:1]
            gains[it, me, s, k : k + 1, stations : 2 * stations] = final[k][1:2]

    def solve():
        weights = meta[0, subs : subs + 1, :]
        for i in range(1, bands):
            weights = weights + meta[i, subs : subs + 1, :]
        index = row_of((1, width), 1).astype(f32)
        abscissa = (2.0 * index + 1.0) / total - 1.0
        terms = [jnp.ones_like(abscissa), abscissa]
        for degree in range(2, DEGREE + 1):
            terms.append(2.0 * abscissa * terms[-1] - terms[-2])
        shape = (ROWS, width)
        cheb = jnp.zeros(shape, f32)
        for c in range(TERMS):
            cheb = jnp.where(row_of(shape) == c, spread(terms[c], shape), cheb)
        right = cheb * weights
        gram = jnp.zeros((ROWS, LANES), f32)
        for c in range(TERMS):
            column = jnp.sum(right * terms[c], axis=1, keepdims=True)
            gram = jnp.where(row_of(gram.shape, 1) == c, column, gram)
        for c in range(TERMS):
            pivot = gram[c : c + 1, c : c + 1]
            gram_row = gram[c : c + 1, :] / pivot
            right_row = right[c : c + 1, :] / pivot
            column = gram[:, c : c + 1]
            gram = jnp.where(row_of(gram.shape) == c, gram_row, gram - column * gram_row)
            right = jnp.where(row_of(shape) == c, right_row, right - column * right_row)
        cheb = jnp.where(row_of(shape) == ROWS - 1, spread(weights, shape), cheb)
        for f in range(total):
            solve_rows[f] = spread(right[:, f : f + 1], (ROWS, stations))
            cheb_rows[f] = spread(cheb[:, f : f + 1], (ROWS, stations))
        return jnp.sum(weights, axis=1, keepdims=True)

    def consensus(it):
        block = (count, stations)
        sums = []
        for half in range(2):
            lanes = slice(half * stations, (half + 1) * stations)

            def project(i, acc):
                for s in range(subs):
                    value = gains[it, i, s, :, lanes]
                    if it > 0:
                        value = value + uall[i, s, :, lanes]
                    f = i * subs + s
                    acc = tuple(
                        acc[c] + spread(solve_rows[f, c : c + 1, :], block) * value
                        for c in range(TERMS)
                    )
                return acc

            coefs = lax.fori_loop(
                0, bands, project, tuple(jnp.zeros(block, f32) for _ in range(TERMS))
            )
            for c in range(TERMS):
                coef[c, :, lanes] = coefs[c]

            def expand(i, acc):
                primal, dual = acc
                for s in range(subs):
                    f = i * subs + s
                    fresh = spread(cheb_rows[f, 0:1, :], block) * coefs[0]
                    for c in range(1, TERMS):
                        fresh = fresh + spread(cheb_rows[f, c : c + 1, :], block) * coefs[c]
                    weight = spread(cheb_rows[f, ROWS - 1 : ROWS, :], block)
                    gap = gains[it, i, s, :, lanes] - fresh
                    if it > 0:
                        moved = fresh - zall[i, s, :, lanes]
                    else:
                        moved = fresh - (1.0 - half)
                    primal = primal + weight * (gap * gap)
                    dual = dual + weight * (moved * moved)
                    if it < ITERS - 1:
                        if it > 0:
                            uall[i, s, :, lanes] = uall[i, s, :, lanes] + gap
                        else:
                            uall[i, s, :, lanes] = gap
                        zall[i, s, :, lanes] = fresh
                return primal, dual

            zero = jnp.zeros(block, f32)
            sums.append(lax.fori_loop(0, bands, expand, (zero, zero)))
        return [
            jnp.sum(sums[0][j] + sums[1][j], axis=(0, 1), keepdims=True) for j in range(2)
        ]

    norm_tile = jnp.zeros((8, LANES), f32)
    weight_sum = None
    for it in range(ITERS):
        for s in range(subs):
            if it == 0:
                build(s)
            sweeps(it, s)
            for distance in range(1, bands):
                gain_copy(it, me, s, distance).start()
        if it == 0:
            for distance in range(1, bands):
                meta_copy(behind(distance), distance).wait_recv()
            weight_sum = solve()
        for s in range(subs):
            for distance in range(1, bands):
                gain_copy(it, behind(distance), s, distance).wait_recv()
        parts = consensus(it)
        for j in range(2):
            norm_tile = jnp.where(
                row_of(norm_tile.shape) == it * 2 + j, parts[j], norm_tile
            )
        if it < ITERS - 1:
            for s in range(subs):
                target = zall[me, s] - uall[me, s]
                for k in range(count):
                    re = spread(target[k : k + 1, 0:stations], tile)
                    im = spread(target[k : k + 1, stations : 2 * stations], tile)
                    ttile[s * count + k] = jnp.where(
                        row == 0, re, jnp.where(row == 1, im, 0.0)
                    )

    norm_all[my_dir] = norm_tile
    for distance in range(1, dirs):
        norm_copy(my_dir, distance).start()

    for s in range(subs):
        wanted = (me * subs + s).astype(f32)
        block = jnp.zeros((count, 2 * stations), f32)
        for distance in sorted({1, bands // 2}):
            source = behind(distance)
            for r in range(subs):
                here = (meta[source, r : r + 1, 0:LANES] == wanted).astype(f32)
                here = spread(here[:, 0:1], block.shape)
                block = block + here * gains[ITERS - 1, source, r]
        delivered[s] = block

    for distance in range(1, dirs):
        norm_copy(lax.rem(my_dir + dirs - distance, dirs), distance).wait_recv()
    sum_tile = norm_all[0]
    for i in range(1, dirs):
        sum_tile = sum_tile + norm_all[i]
    norms[...] = jnp.sqrt(sum_tile / (count * dirs * 2.0 * stations * weight_sum))

    for distance in range(1, dirs):
        norm_copy(my_dir, distance).wait_send()
    for distance in range(1, bands):
        meta_copy(me, distance).wait_send()
        for it in range(ITERS):
            for s in range(subs):
                gain_copy(it, me, s, distance).wait_send()


def per_device(bands, dirs, visibilities, sky_model, rfi_flags, destination):
    subs, count, _, stations, _ = visibilities.shape
    pairs = subs * count
    total = bands * subs
    width = -(-total // LANES) * LANES
    meta_rows = -(-(subs + 1) // 8) * 8
    vmem = pl.BlockSpec(memory_space=pltpu.VMEM)
    hbm = pl.BlockSpec(memory_space=pl.ANY)
    sem = pltpu.SemaphoreType.DMA
    delivered, coefficients, norms = pl.pallas_call(
        functools.partial(kernel, bands, dirs),
        out_shape=(
            jax.ShapeDtypeStruct((subs, count, 2 * stations), f32),
            jax.ShapeDtypeStruct((TERMS, count, 2 * stations), f32),
            jax.ShapeDtypeStruct((8, LANES), f32),
        ),
        in_specs=[hbm, hbm, vmem, pl.BlockSpec(memory_space=pltpu.SMEM)],
        out_specs=(vmem, vmem, vmem),
        scratch_shapes=[
            pltpu.VMEM((pairs, 2, stations, stations), bf16),
            pltpu.VMEM((pairs, 2, stations, stations), bf16),
            pltpu.VMEM((pairs, 6 * stations, stations), bf16),
            pltpu.VMEM((2, 4, stations, stations), f32),
            pltpu.VMEM((subs, stations, stations), f32),
            pltpu.VMEM((subs, 8, stations), f32),
            pltpu.VMEM((bands, meta_rows, width), f32),
            pltpu.VMEM((ITERS, bands, subs, count, 2 * stations), f32),
            pltpu.VMEM((bands, subs, count, 2 * stations), f32),
            pltpu.VMEM((bands, subs, count, 2 * stations), f32),
            pltpu.VMEM((pairs, 8, stations), f32),
            pltpu.VMEM((pairs, 8, stations), f32),
            pltpu.VMEM((total, ROWS, stations), f32),
            pltpu.VMEM((total, ROWS, stations), f32),
            pltpu.VMEM((dirs, 8, LANES), f32),
            sem((pairs,)),
            sem((pairs,)),
            sem((bands,)),
            sem((bands,)),
            sem((ITERS, subs, bands)),
            sem((ITERS, subs, bands)),
            sem((dirs,)),
            sem((dirs,)),
        ],
        compiler_params=pltpu.CompilerParams(
            collective_id=0, has_side_effects=True, vmem_limit_bytes=56 * 1024 * 1024
        ),
    )(visibilities, sky_model, rfi_flags, destination)
    shape = (count, 2, stations)
    return (
        delivered.reshape((subs,) + shape),
        coefficients.reshape((TERMS,) + shape),
        norms[: 2 * ITERS, 0].reshape(ITERS, 2),
    )


def solution(mesh):
    return jax.shard_map(
        functools.partial(per_device, mesh.shape["band"], mesh.shape["dir"]),
        mesh=mesh,
        in_specs=(
            P("band", "dir", None, None, None),
            P("band", "dir", None, None, None),
            P("band", None, None),
            P("band"),
        ),
        out_specs=(P("band", "dir", None, None), P(None, "dir", None, None), P()),
        check_vma=False,
    )
```

```python
import functools

import jax
import jax.numpy as jnp
from jax import lax
from jax.experimental import pallas as pl
from jax.experimental.pallas import tpu as pltpu
from jax.sharding import PartitionSpec as P

BLOCK = 32
DEGREE = 8
SWEEPS = 4
ITERS = 2
TERMS = DEGREE + 1
ROWS = 16
LANES = 128

penalty_share = 0.4
f32 = jnp.float32
bf16 = jnp.bfloat16
MESH = pl.DeviceIdType.MESH


def row_of(shape, axis=0):
    return lax.broadcasted_iota(jnp.int32, shape, axis)


def spread(value, shape):
    return jnp.broadcast_to(value, shape)


def left_side(gain):
    row = row_of(gain.shape)
    part = lax.rem(row, 4)
    re = spread(gain[0:1], gain.shape)
    im = spread(gain[1:2], gain.shape)
    zero = jnp.zeros_like(gain)
    first = jnp.where(part == 0, re, jnp.where(part == 1, im, zero))
    second = jnp.where(part == 0, -im, jnp.where(part == 1, re, zero))
    third = jnp.where(part == 2, re * re + im * im, zero)
    sides = []
    for full in (first, second, third):
        lead = full.astype(bf16).astype(f32)
        sides.append(jnp.where(row < 4, lead, full - lead).astype(bf16))
    return jnp.concatenate(sides + sides, axis=1)


def kernel(
    bands,
    dirs,
    vis_hbm,
    sky_hbm,
    flags,
    dest,
    delivered,
    coef,
    norms,
    vis,
    sky,
    oper,
    turned,
    keep,
    wpen,
    meta,
    gains,
    zall,
    uall,
    gtile,
    ttile,
    solve_rows,
    cheb_rows,
    norm_all,
    vis_sem,
    sky_sem,
    meta_send,
    meta_recv,
    gain_send,
    gain_recv,
    norm_send,
    norm_recv,
):
    subs, count, _, stations, _ = vis_hbm.shape
    blocks = flags.shape[-1]
    total = bands * subs
    width = meta.shape[-1]
    me = lax.axis_index("band")
    my_dir = lax.axis_index("dir")
    tile = (8, stations)

    def ahead(distance):
        return lax.rem(me + distance, bands)

    def behind(distance):
        return lax.rem(me + bands - distance, bands)

    def load(pair):
        s, k = divmod(pair, count)
        return (
            pltpu.make_async_copy(vis_hbm.at[s, k], vis.at[pair], vis_sem.at[pair]),
            pltpu.make_async_copy(sky_hbm.at[s, k], sky.at[pair], sky_sem.at[pair]),
        )

    for pair in range(subs * count):
        for copy in load(pair):
            copy.start()

    barrier = pltpu.get_barrier_semaphore()
    for distance in range(1, bands):
        pl.semaphore_signal(
            barrier, inc=1, device_id={"band": ahead(distance)}, device_id_type=MESH
        )
    for distance in range(1, dirs):
        pl.semaphore_signal(
            barrier,
            inc=1,
            device_id={"dir": lax.rem(my_dir + distance, dirs)},
            device_id_type=MESH,
        )

    lane_w = row_of((1, width), 1)
    weight_row = jnp.zeros((1, width), f32)
    dest_rows = []
    for s in range(subs):
        kept = (1 - flags[s]).astype(f32)
        weight = (1.0 + jnp.sum(kept, axis=(0, 1), keepdims=True)) / (1.0 + blocks * blocks)
        wpen[s] = spread(penalty_share * stations * weight, tile)
        weight_row = jnp.where(lane_w == me * subs + s, weight, weight_row)
        dest_rows.append(jnp.full((1, width), dest[s], jnp.int32).astype(f32))
        lane = row_of((1, stations), 1) // BLOCK
        for i in range(blocks):
            shape = (BLOCK, stations)
            across = jnp.zeros((1, stations), f32)
            for j in range(blocks):
                across = jnp.where(lane == j, kept[j : j + 1, i : i + 1], across)
            apart = row_of(shape) + i * BLOCK != row_of(shape, 1)
            keep[s, i * BLOCK : (i + 1) * BLOCK, :] = jnp.where(
                apart, spread(across, shape), 0.0
            )
    meta[me] = jnp.zeros(meta.shape[1:], f32)
    for s in range(subs):
        meta[me, s : s + 1, :] = dest_rows[s]
    meta[me, subs : subs + 1, :] = weight_row

    row = row_of(tile)
    for pair in range(subs * count):
        ttile[pair] = jnp.where(row == 0, 1.0, jnp.zeros(tile, f32))

    pl.semaphore_wait(barrier, bands - 1 + dirs - 1)

    def meta_copy(slot, distance):
        return pltpu.make_async_remote_copy(
            src_ref=meta.at[slot],
            dst_ref=meta.at[slot],
            send_sem=meta_send.at[distance],
            recv_sem=meta_recv.at[distance],
            device_id={"band": ahead(distance)},
            device_id_type=MESH,
        )

    def gain_copy(it, slot, s, distance):
        return pltpu.make_async_remote_copy(
            src_ref=gains.at[it, slot, s],
            dst_ref=gains.at[it, slot, s],
            send_sem=gain_send.at[it, s, distance],
            recv_sem=gain_recv.at[it, s, distance],
            device_id={"band": ahead(distance)},
            device_id_type=MESH,
        )

    def norm_copy(slot, distance):
        return pltpu.make_async_remote_copy(
            src_ref=norm_all.at[slot],
            dst_ref=norm_all.at[slot],
            send_sem=norm_send.at[distance],
            recv_sem=norm_recv.at[distance],
            device_id={"dir": lax.rem(my_dir + distance, dirs)},
            device_id_type=MESH,
        )

    for distance in range(1, bands):
        meta_copy(me, distance).start()

    square = (stations, stations)
    identity = (row_of(square) == row_of(square, 1)).astype(f32).astype(bf16)

    def build(s):
        def one(k, carry):
            pair = s * count + k
            pltpu.make_async_copy(vis_hbm.at[s, k], vis.at[pair], vis_sem.at[pair]).wait()
            pltpu.make_async_copy(sky_hbm.at[s, k], sky.at[pair], sky_sem.at[pair]).wait()
            slot = lax.rem(k, 2)
            for part, source in enumerate((vis, sky)):
                for j in range(2):
                    turned[slot, 2 * part + j] = lax.dot_general(
                        identity,
                        source[pair, j],
                        (((1,), (1,)), ((), ())),
                        preferred_element_type=f32,
                    )
            sums = [jnp.zeros(tile, f32) for _ in range(3)]
            for i in range(stations // BLOCK):
                rows = slice(i * BLOCK, (i + 1) * BLOCK)
                baseline = keep[s, rows, :]
                data_re = turned[slot, 0, rows, :]
                data_im = turned[slot, 1, rows, :]
                model_re = turned[slot, 2, rows, :]
                model_im = turned[slot, 3, rows, :]
                parts = (
                    baseline * (model_re * data_re + model_im * data_im),
                    baseline * (model_re * data_im - model_im * data_re),
                    baseline * (model_re * model_re + model_im * model_im),
                )
                for j, full in enumerate(parts):
                    for r in range(0, BLOCK, 8):
                        sums[j] = sums[j] + full[r : r + 8]
                    lead = full.astype(bf16)
                    base = j * stations + i * BLOCK
                    oper[pair, base : base + BLOCK, :] = lead
                    base = base + 3 * stations
                    oper[pair, base : base + BLOCK, :] = (full - lead.astype(f32)).astype(bf16)
            re, im, mag = (spread(jnp.sum(x, axis=0, keepdims=True), tile) for x in sums)
            out = jnp.where(row == 0, re, jnp.where(row == 1, im, 0.0))
            penalty = wpen[s]
            gtile[pair] = (out + penalty * ttile[pair]) / (mag + penalty)
            return carry

        lax.fori_loop(0, count, one, 0, unroll=2)

    def sweeps(it, s):
        penalty = wpen[s]

        def one(index, held):
            step = jnp.where(lax.rem(index, 2) == 1, 0.5, 1.0).astype(f32)
            fresh = []
            for k in range(count):
                pair = s * count + k
                gain = held[k]
                out = lax.dot_general(
                    left_side(gain),
                    oper[pair],
                    (((1,), (0,)), ((), ())),
                    preferred_element_type=f32,
                )
                out = out + pltpu.roll(out, 4, 0)
                updated = (out + penalty * ttile[pair]) / (spread(out[2:3], tile) + penalty)
                fresh.append(step * updated + (1.0 - step) * gain)
            return tuple(fresh)

        start = tuple(gtile[s * count + k] for k in range(count))
        final = lax.fori_loop(1 if it == 0 else 0, SWEEPS, one, start)
        for k in range(count):
            gtile[s * count + k] = final[k]
            gains[it, me, s, k : k + 1, 0:stations] = final[k][0:1]
            gains[it, me, s, k : k + 1, stations : 2 * stations] = final[k][1:2]

    def solve():
        weights = meta[0, subs : subs + 1, :]
        for i in range(1, bands):
            weights = weights + meta[i, subs : subs + 1, :]
        index = row_of((1, width), 1).astype(f32)
        abscissa = (2.0 * index + 1.0) / total - 1.0
        terms = [jnp.ones_like(abscissa), abscissa]
        for degree in range(2, DEGREE + 1):
            terms.append(2.0 * abscissa * terms[-1] - terms[-2])
        shape = (ROWS, width)
        cheb = jnp.zeros(shape, f32)
        for c in range(TERMS):
            cheb = jnp.where(row_of(shape) == c, spread(terms[c], shape), cheb)
        right = cheb * weights
        gram = jnp.zeros((ROWS, LANES), f32)
        for c in range(TERMS):
            column = jnp.sum(right * terms[c], axis=1, keepdims=True)
            gram = jnp.where(row_of(gram.shape, 1) == c, column, gram)
        for c in range(TERMS):
            pivot = gram[c : c + 1, c : c + 1]
            gram_row = gram[c : c + 1, :] / pivot
            right_row = right[c : c + 1, :] / pivot
            column = gram[:, c : c + 1]
            gram = jnp.where(row_of(gram.shape) == c, gram_row, gram - column * gram_row)
            right = jnp.where(row_of(shape) == c, right_row, right - column * right_row)
        cheb = jnp.where(row_of(shape) == ROWS - 1, spread(weights, shape), cheb)
        for f in range(total):
            solve_rows[f] = spread(right[:, f : f + 1], (ROWS, stations))
            cheb_rows[f] = spread(cheb[:, f : f + 1], (ROWS, stations))
        return jnp.sum(weights, axis=1, keepdims=True)

    def consensus(it):
        block = (count, stations)
        sums = []
        for half in range(2):
            lanes = slice(half * stations, (half + 1) * stations)

            def project(i, acc):
                for s in range(subs):
                    value = gains[it, i, s, :, lanes]
                    if it > 0:
                        value = value + uall[i, s, :, lanes]
                    f = i * subs + s
                    acc = tuple(
                        acc[c] + spread(solve_rows[f, c : c + 1, :], block) * value
                        for c in range(TERMS)
                    )
                return acc

            coefs = lax.fori_loop(
                0, bands, project, tuple(jnp.zeros(block, f32) for _ in range(TERMS))
            )
            if it == ITERS - 1:
                for c in range(TERMS):
                    for k in range(count):
                        coef[c, k, half : half + 1, :] = coefs[c][k : k + 1]

            def expand(i, acc):
                primal, dual = acc
                for s in range(subs):
                    f = i * subs + s
                    fresh = spread(cheb_rows[f, 0:1, :], block) * coefs[0]
                    for c in range(1, TERMS):
                        fresh = fresh + spread(cheb_rows[f, c : c + 1, :], block) * coefs[c]
                    weight = spread(cheb_rows[f, ROWS - 1 : ROWS, :], block)
                    gap = gains[it, i, s, :, lanes] - fresh
                    if it > 0:
                        moved = fresh - zall[i, s, :, lanes]
                    else:
                        moved = fresh - (1.0 - half)
                    primal = primal + weight * (gap * gap)
                    dual = dual + weight * (moved * moved)
                    if it < ITERS - 1:
                        if it > 0:
                            uall[i, s, :, lanes] = uall[i, s, :, lanes] + gap
                        else:
                            uall[i, s, :, lanes] = gap
                        zall[i, s, :, lanes] = fresh
                return primal, dual

            zero = jnp.zeros(block, f32)
            sums.append(lax.fori_loop(0, bands, expand, (zero, zero)))
        return [
            jnp.sum(sums[0][j] + sums[1][j], axis=(0, 1), keepdims=True) for j in range(2)
        ]

    norm_tile = jnp.zeros((8, LANES), f32)
    weight_sum = None
    for it in range(ITERS):
        for s in range(subs):
            if it == 0:
                build(s)
            sweeps(it, s)
            for distance in range(1, bands):
                gain_copy(it, me, s, distance).start()
        if it == 0:
            for distance in range(1, bands):
                meta_copy(behind(distance), distance).wait_recv()
            weight_sum = solve()
        for s in range(subs):
            for distance in range(1, bands):
                gain_copy(it, behind(distance), s, distance).wait_recv()
        parts = consensus(it)
        for j in range(2):
            norm_tile = jnp.where(
                (row_of(norm_tile.shape) == it) & (row_of(norm_tile.shape, 1) == j),
                parts[j],
                norm_tile,
            )
        if it < ITERS - 1:
            for s in range(subs):
                target = zall[me, s] - uall[me, s]
                for k in range(count):
                    re = spread(target[k : k + 1, 0:stations], tile)
                    im = spread(target[k : k + 1, stations : 2 * stations], tile)
                    ttile[s * count + k] = jnp.where(
                        row == 0, re, jnp.where(row == 1, im, 0.0)
                    )

    norm_all[my_dir] = norm_tile
    for distance in range(1, dirs):
        norm_copy(my_dir, distance).start()

    for s in range(subs):
        wanted = (me * subs + s).astype(f32)
        block = jnp.zeros((count, 2 * stations), f32)
        for distance in sorted({1, bands // 2}):
            source = behind(distance)
            for r in range(subs):
                here = (meta[source, r : r + 1, 0:LANES] == wanted).astype(f32)
                here = spread(here[:, 0:1], block.shape)
                block = block + here * gains[ITERS - 1, source, r]
        for k in range(count):
            delivered[s, k, 0:1, :] = block[k : k + 1, 0:stations]
            delivered[s, k, 1:2, :] = block[k : k + 1, stations : 2 * stations]

    for distance in range(1, dirs):
        norm_copy(lax.rem(my_dir + dirs - distance, dirs), distance).wait_recv()
    sum_tile = norm_all[0]
    for i in range(1, dirs):
        sum_tile = sum_tile + norm_all[i]
    final = jnp.sqrt(sum_tile / (count * dirs * 2.0 * stations * weight_sum))
    norms[...] = final[0:ITERS, 0:2]

    for distance in range(1, dirs):
        norm_copy(my_dir, distance).wait_send()
    for distance in range(1, bands):
        meta_copy(me, distance).wait_send()
        for it in range(ITERS):
            for s in range(subs):
                gain_copy(it, me, s, distance).wait_send()


def per_device(bands, dirs, visibilities, sky_model, rfi_flags, destination):
    subs, count, _, stations, _ = visibilities.shape
    pairs = subs * count
    total = bands * subs
    width = -(-total // LANES) * LANES
    meta_rows = -(-(subs + 1) // 8) * 8
    vmem = pl.BlockSpec(memory_space=pltpu.VMEM)
    hbm = pl.BlockSpec(memory_space=pl.ANY)
    sem = pltpu.SemaphoreType.DMA
    delivered, coefficients, norms = pl.pallas_call(
        functools.partial(kernel, bands, dirs),
        out_shape=(
            jax.ShapeDtypeStruct((subs, count, 2, stations), f32),
            jax.ShapeDtypeStruct((TERMS, count, 2, stations), f32),
            jax.ShapeDtypeStruct((ITERS, 2), f32),
        ),
        in_specs=[hbm, hbm, vmem, pl.BlockSpec(memory_space=pltpu.SMEM)],
        out_specs=(vmem, vmem, vmem),
        scratch_shapes=[
            pltpu.VMEM((pairs, 2, stations, stations), bf16),
            pltpu.VMEM((pairs, 2, stations, stations), bf16),
            pltpu.VMEM((pairs, 6 * stations, stations), bf16),
            pltpu.VMEM((2, 4, stations, stations), f32),
            pltpu.VMEM((subs, stations, stations), f32),
            pltpu.VMEM((subs, 8, stations), f32),
            pltpu.VMEM((bands, meta_rows, width), f32),
            pltpu.VMEM((ITERS, bands, subs, count, 2 * stations), f32),
            pltpu.VMEM((bands, subs, count, 2 * stations), f32),
            pltpu.VMEM((bands, subs, count, 2 * stations), f32),
            pltpu.VMEM((pairs, 8, stations), f32),
            pltpu.VMEM((pairs, 8, stations), f32),
            pltpu.VMEM((total, ROWS, stations), f32),
            pltpu.VMEM((total, ROWS, stations), f32),
            pltpu.VMEM((dirs, 8, LANES), f32),
            sem((pairs,)),
            sem((pairs,)),
            sem((bands,)),
            sem((bands,)),
            sem((ITERS, subs, bands)),
            sem((ITERS, subs, bands)),
            sem((dirs,)),
            sem((dirs,)),
        ],
        compiler_params=pltpu.CompilerParams(
            collective_id=0, has_side_effects=True, vmem_limit_bytes=56 * 1024 * 1024
        ),
    )(visibilities, sky_model, rfi_flags, destination)
    return delivered, coefficients, norms


def solution(mesh):
    return jax.shard_map(
        functools.partial(per_device, mesh.shape["band"], mesh.shape["dir"]),
        mesh=mesh,
        in_specs=(
            P("band", "dir", None, None, None),
            P("band", "dir", None, None, None),
            P("band", None, None),
            P("band"),
        ),
        out_specs=(P("band", "dir", None, None), P(None, "dir", None, None), P()),
        check_vma=False,
    )
```
